32 devices in a mesh: seq: 8 (over z, y), dp: 4 (over x, core).
Axes of the slice: x: 2, y: 2, z: 4, core: 2. Of those that a mesh axis runs over, the one named last changes fastest.
Arguments:
- hidden: bfloat16 [4, 2048, 4608], P('dp', 'seq'), may hold values from -6 to 6
- queries: bfloat16 [4, 2048, 2048], P('dp', 'seq'), may hold values from -64 to 64
- down_weight: bfloat16 [4608, 1024], P('dp'), may hold values from -0.09375 to 0.09375
- up_weight: bfloat16 [2, 512, 1024], P(None, 'dp'), may hold values from -0.25 to 0.25
- lengths: int32 [4], P('dp'), may hold values from 512 to 2048
Outputs:
- latent_cache: bfloat16 [4, 2048, 1024], P('dp', 'seq')
- attended: bfloat16 [4, 2048, 2048], P('dp', 'seq')
The draws below stay inside these ranges and needn't reach their ends.
All inputs are finite; a program needn't handle non-finite values.
Results may differ from the reference program's by a relative error of at most 0.012.
The reference program's roundings to bfloat16 on the way count: a program that leaves them out, or rounds other values in their place, can miss the bound.
Values may be sent and summed in bfloat16 or wider, within the bound.
A program may use at most 128 MiB of HBM per device.

```python
import math
import jax
import jax.numpy as jnp
from jax import lax

D = 4608
HEAD = 128
Q_HEADS = 16
KV_HEADS = 8
RANK = 1024
WINDOW = 4096
SEQ = 2048
BATCH = 4


def draw_queries(key, part):
    base_key = jax.random.fold_in(key, 11)
    entry_key, scale_key = jax.random.split(base_key)
    entries = jnp.clip(jax.random.normal(entry_key, (BATCH, SEQ, Q_HEADS, HEAD), jnp.float32), -4.0, 4.0)
    lowest, highest = (0.5, 16.0)
    log_scales = jax.random.uniform(scale_key, (BATCH, SEQ, Q_HEADS, 1), jnp.float32, math.log(lowest), math.log(highest))
    scaled = entries * jnp.exp(log_scales)
    return scaled.reshape(BATCH, SEQ, Q_HEADS * HEAD).astype(jnp.bfloat16)


def plant(drawn, stream_key, low, largest):
    extent = drawn.shape
    place = [jax.random.randint(jax.random.fold_in(stream_key, axis), (), 0, extent[axis]) for axis in range(len(extent))]
    drawn = drawn.at[tuple(place)].set(low)
    longest = extent.index(max(extent))
    place[longest] = (place[longest] + 1) % extent[longest]
    return drawn.at[tuple(place)].set(largest)


def block_levels(stream_key, extent, pieces, least, high):
    gain, own = 1.0, jax.random.fold_in(stream_key, 6)
    for dim, parts in pieces:
        steps = jnp.exp(jax.random.uniform(jax.random.fold_in(own, dim), (parts,), jnp.float32, least / len(pieces), high / len(pieces)))
        gain = gain * jnp.repeat(steps, extent[dim] // parts).reshape([-1 if axis == dim else 1 for axis in range(len(extent))])
    return gain


def bell_draw(rng, shape, scale, bound, pieces=(), kind=jnp.bfloat16):
    values = jax.random.normal(rng, shape, jnp.float32) * scale
    if len(pieces) > 0:
        values = block_levels(rng, shape, pieces, -0.22, 0.18) * values
    return jnp.clip(values, min=-bound, max=bound).astype(kind)


def setup_inputs(seed: int = 0) -> dict:
    arg_keys = jax.random.split(jax.random.key(seed), 6)
    return {
        "hidden": bell_draw(arg_keys[0], (BATCH, SEQ, D), 1.0, 6.0, ((0, 4), (1, 8))),
        "queries": draw_queries(jax.random.fold_in(arg_keys[5], 71), 0),
        "down_weight": bell_draw(arg_keys[2], (D, RANK), D ** -0.5, 0.09375, ((0, 4),)),
        "up_weight": bell_draw(arg_keys[3], (2, RANK // 2, KV_HEADS * HEAD), (RANK // 2) ** -0.5, 0.25, ((1, 4),)),
        "lengths": plant(jax.random.randint(arg_keys[4], (BATCH,), SEQ // 4, SEQ + 1), jax.random.fold_in(arg_keys[4], 1), SEQ // 4, SEQ).astype(jnp.int32),
    }


query_scale = 144.0 ** -0.5
soft_cap = 50.0


def rotate(values_in, start_pos):
    batches, count, width = values_in.shape
    half_head = HEAD // 2
    places = (start_pos + jnp.arange(count, dtype=jnp.int32)).astype(jnp.float32)
    freqs = 10000.0 ** (-2.0 * jnp.arange(half_head, dtype=jnp.float32) / HEAD)
    angles = places[:, None] * freqs[None, :]
    cosine = jnp.cos(angles)[None, :, None, :]
    sine_val = jnp.sin(angles)[None, :, None, :]
    split_heads = values_in.reshape(batches, count, width // HEAD, 2, half_head)
    lower = split_heads[:, :, :, 0, :]
    upper = split_heads[:, :, :, 1, :]
    turned = jnp.stack([lower * cosine - upper * sine_val, upper * cosine + lower * sine_val], axis=3)
    return turned.reshape(batches, count, width)


def reference(hidden, queries, down_weight, up_weight, lengths):
    flat_hidden = hidden.reshape(BATCH * SEQ, D)
    latent = jnp.dot(flat_hidden, down_weight, preferred_element_type=jnp.float32).astype(jnp.bfloat16)
    latent = latent.reshape(BATCH, SEQ, RANK)
    positions = jnp.arange(SEQ, dtype=jnp.int32)
    is_live = positions[None, :] < lengths[:, None]
    latent = jnp.where(is_live[:, :, None], latent, jnp.zeros((), jnp.bfloat16))
    key_rank = RANK // 2
    kv_width = KV_HEADS * HEAD
    keys_raw = jnp.dot(latent[:, :, :key_rank].reshape(-1, key_rank), up_weight[0], preferred_element_type=jnp.float32)
    keys_all = rotate(keys_raw.reshape(BATCH, SEQ, kv_width), 0).astype(jnp.bfloat16)
    values_all = jnp.dot(latent[:, :, key_rank:].reshape(-1, key_rank), up_weight[1], preferred_element_type=jnp.float32)
    values_all = values_all.astype(jnp.bfloat16).reshape(BATCH, SEQ, kv_width)
    block_rows = math.gcd(512, SEQ)
    blocks = SEQ // block_rows
    padding = jnp.zeros((BATCH, WINDOW, kv_width), jnp.bfloat16)
    keys_pad = jnp.concatenate([padding, keys_all], axis=1)
    values_pad = jnp.concatenate([padding, values_all], axis=1)
    query_width = Q_HEADS * HEAD
    ratio = Q_HEADS // KV_HEADS

    def one_block(flat_index):
        batch_index = (flat_index // blocks).astype(jnp.int32)
        row_start = ((flat_index % blocks) * block_rows).astype(jnp.int32)
        zero_idx = jnp.zeros((), jnp.int32)
        keys_win = lax.dynamic_slice(keys_pad, (batch_index, row_start, zero_idx), (1, WINDOW + block_rows, kv_width))[0]
        values_win = lax.dynamic_slice(values_pad, (batch_index, row_start, zero_idx), (1, WINDOW + block_rows, kv_width))[0]
        query_blk = lax.dynamic_slice(queries, (batch_index, row_start, zero_idx), (1, block_rows, query_width))[0]
        q_split = query_blk.astype(jnp.float32).reshape(block_rows, KV_HEADS, ratio, HEAD)
        keys_grp = keys_win.astype(jnp.float32).reshape(-1, KV_HEADS, HEAD)
        values_grp = values_win.astype(jnp.float32).reshape(-1, KV_HEADS, HEAD)
        raw = jnp.einsum("lgrd,ngd->grln", q_split, keys_grp, precision=lax.Precision.HIGHEST)
        capped = soft_cap * jnp.tanh(raw * (query_scale / soft_cap))
        q_pos = row_start + jnp.arange(block_rows, dtype=jnp.int32)
        key_pos = row_start - WINDOW + jnp.arange(WINDOW + block_rows, dtype=jnp.int32)
        allowed = (key_pos[None, :] <= q_pos[:, None]) & (key_pos[None, :] > q_pos[:, None] - WINDOW) & (key_pos[None, :] >= 0)
        expo = jnp.where(allowed, jnp.exp(capped), 0.0)
        denom = jnp.sum(expo, axis=-1)
        probs = expo.astype(jnp.bfloat16).astype(jnp.float32)
        numer = jnp.einsum("grln,ngd->lgrd", probs, values_grp, precision=lax.Precision.HIGHEST)
        result = numer / jnp.transpose(denom, (2, 0, 1))[..., None]
        result = result.reshape(block_rows, query_width)
        live_rows = q_pos < lengths[batch_index]
        return jnp.where(live_rows[:, None], result, 0.0).astype(jnp.bfloat16)

    outputs = lax.map(one_block, jnp.arange(BATCH * blocks, dtype=jnp.int32))
    attended = outputs.reshape(BATCH, SEQ, query_width)
    return latent, attended
```

```python
import functools
import math

import jax
import jax.numpy as jnp
import numpy as np
from jax import lax
from jax.experimental import pallas as pl
from jax.experimental.pallas import tpu as pltpu
from jax.sharding import PartitionSpec as P

HEAD = 128
WINDOW = 4096
MESH = pl.DeviceIdType.MESH

query_scale = 144.0 ** (-0.5)
soft_cap = 50.0
EXP_SCALE = soft_cap * math.log2(math.e)


def angle_tables(rows, blocks):
    half = HEAD // 2
    freqs = 10000.0 ** (-2.0 * np.arange(half, dtype=np.float64) / HEAD)
    freqs = np.concatenate([freqs, freqs])[None, :]
    sign = np.concatenate([-np.ones(half), np.ones(half)])[None, :]
    near = np.arange(rows, dtype=np.float64)[:, None] * freqs
    far = (rows * np.arange(blocks, dtype=np.float64))[:, None] * freqs
    near = np.stack([np.cos(near), sign * np.sin(near)]).astype(np.float32)
    far = np.stack([np.cos(far), sign * np.sin(far)]).astype(np.float32)
    return near, far


def piece_count(half):
    for pieces in (6, 5, 4, 3, 2):
        if half % (pieces * 16) == 0:
            return pieces
    return 1


def kernel(
    ring, pieces, lengths_ref, hidden_ref, q_ref, down_ref, up_ref, near_ref, far_ref,
    latent_out, attended_out,
    hid, q_raw, qs, wf, up, lat, acc, keys, values, numer, denom, out_buf,
    local_sem, x_send, x_recv, y_send, y_recv, c_send, c_recv, own_send, own_recv,
    up_send, up_recv, chain_send, pair_send, lat_recv, out_sem,
):
    seq = lax.axis_index("seq")
    dp = lax.axis_index("dp")
    rows = lat.shape[1]
    shard = down_ref.shape[0]
    half = shard // 2
    piece = half // pieces
    up_rows = up_ref.shape[1]
    groups = qs.shape[0]
    ratio = qs.shape[1] // rows
    key_rank = lat.shape[2] // 2
    total = ring * rows

    side = lax.rem(seq, 2)
    pair = seq + 1 - 2 * side
    core = lax.rem(dp, 2)
    mate = dp + 1 - 2 * core
    across = lax.rem(dp + 2, 4)
    diagonal = lax.rem(mate + 2, 4)
    has_next = seq + 2 < ring
    has_prev = seq >= 2

    def local(src, dst, sem):
        return pltpu.make_async_copy(src, dst, sem)

    loads = [
        local(down_ref, wf.at[dp], local_sem.at[0]),
        local(hidden_ref.at[0], hid, local_sem.at[1]),
        local(up_ref, up.at[:, pl.ds(pl.multiple_of(dp * up_rows, up_rows), up_rows), :], local_sem.at[2]),
        local(q_ref.at[0], q_raw, local_sem.at[3]),
    ]
    for load in loads:
        load.start()

    barrier = pltpu.get_barrier_semaphore()

    def greet(device):
        pl.semaphore_signal(barrier, inc=1, device_id=device, device_id_type=MESH)

    greet({"seq": seq, "dp": mate})
    greet({"seq": seq, "dp": across})
    greet({"seq": pair, "dp": dp})

    @pl.when(has_next)
    def _():
        greet({"seq": seq + 2, "dp": dp})

    @pl.when(has_prev)
    def _():
        greet({"seq": seq - 2, "dp": dp})

    pl.semaphore_wait(barrier, 3 + has_next.astype(jnp.int32) + has_prev.astype(jnp.int32))

    def remote(src, dst, send, recv, device):
        return pltpu.make_async_remote_copy(
            src_ref=src, dst_ref=dst, send_sem=send, recv_sem=recv, device_id=device, device_id_type=MESH
        )

    to_mate = {"seq": seq, "dp": mate}
    to_across = {"seq": seq, "dp": across}
    to_pair = {"seq": pair, "dp": dp}
    to_next = {"seq": lax.rem(seq + 2, ring), "dp": dp}

    def part(which, index):
        return pl.ds(pl.multiple_of(which * half + index * piece, 16), piece)

    def x_copy(index):
        return remote(
            down_ref.at[part(side, index)], wf.at[dp, part(side, index)],
            x_send.at[index], x_recv.at[index], to_across,
        )

    def y_copy(index):
        view = wf.at[across, part(side, index)]
        return remote(view, view, y_send.at[index], y_recv.at[index], to_pair)

    def c_copy(slot, which, index):
        view = wf.at[across, part(which, index)]
        return remote(view, view, c_send.at[slot, index], c_recv.at[slot, index], to_mate)

    x_copies = [x_copy(i) for i in range(pieces)]
    for copy in x_copies:
        copy.start()
    own_copy = remote(down_ref, wf.at[dp], own_send, own_recv, to_mate)
    own_copy.start()

    def up_view(owner):
        return up.at[:, pl.ds(pl.multiple_of(owner * up_rows, up_rows), up_rows), :]

    up_across = remote(up_ref, up_view(dp), up_send.at[0], up_recv.at[0], to_across)
    up_across.start()
    up_mate = remote(up_ref, up_view(dp), up_send.at[1], up_recv.at[1], to_mate)
    up_mate.start()

    loads[3].wait()
    for g in range(groups):
        for r in range(ratio):
            column = (g * ratio + r) * HEAD
            qs[g, r * rows : (r + 1) * rows, :] = q_raw[:, column : column + HEAD]
    numer[...] = jnp.zeros_like(numer)
    denom[...] = jnp.zeros_like(denom)

    def project(owner):
        columns = pl.ds(pl.multiple_of(owner * shard, 128), shard)
        return jnp.dot(hid[:, columns], wf[owner], preferred_element_type=jnp.float32)

    loads[1].wait()
    loads[0].wait()
    acc[...] = project(dp)

    y_copies = [y_copy(i) for i in range(pieces)]
    near_copies = [c_copy(0, side, i) for i in range(pieces)]
    far_copies = [c_copy(1, 1 - side, i) for i in range(pieces)]
    for i in range(pieces):
        x_copies[i].wait_recv()
        y_copies[i].start()
        near_copies[i].start()
        if i >= 1:
            y_copies[i - 1].wait_recv()
            far_copies[i - 1].start()
        if i == pieces - 1:
            own_copy.wait_recv()
            acc[...] += project(mate)
    y_copies[pieces - 1].wait_recv()
    far_copies[pieces - 1].start()
    acc[...] += project(across)
    for i in range(pieces):
        near_copies[i].wait_recv()
        far_copies[i].wait_recv()
    live_count = lengths_ref[0] - seq * rows
    total_rows = acc[...] + project(diagonal)
    live = lax.broadcasted_iota(jnp.int32, total_rows.shape, 0) < live_count
    lat[seq] = jnp.where(live, total_rows, 0.0).astype(jnp.bfloat16)

    def chain(block):
        view = lat.at[block]
        return remote(view, view, chain_send.at[block], lat_recv.at[block], to_next)

    def swap(block):
        view = lat.at[block]
        return remote(view, view, pair_send.at[block], lat_recv.at[block], to_pair)

    @pl.when(has_next)
    def _():
        chain(seq).start()

    @pl.when(side == 0)
    def _():
        swap(seq).start()

    latent_copy = local(lat.at[seq], latent_out.at[0], out_sem.at[groups])
    latent_copy.start()

    up_mate.wait_recv()
    up_across.wait_recv()
    up_relay = remote(up_view(across), up_view(across), up_send.at[2], up_recv.at[2], to_mate)
    up_relay.start()
    loads[2].wait()
    up_relay.wait_recv()

    def attend(block, distance, masked):
        latent = lat[block]
        near_cos, near_sin = near_ref[0], near_ref[1]
        far_cos = far_ref[0, pl.ds(block, 1), :]
        far_sin = far_ref[1, pl.ds(block, 1), :]
        cosine = near_cos * far_cos - near_sin * far_sin
        sine = near_sin * far_cos + near_cos * far_sin
        keys_raw = jnp.dot(latent[:, :key_rank], up[0], preferred_element_type=jnp.float32)
        for g in range(groups):
            head = keys_raw[:, g * HEAD : (g + 1) * HEAD]
            turned = head * cosine + pltpu.roll(head, HEAD // 2, 1) * sine
            keys[g] = turned.astype(jnp.bfloat16)
        values_raw = jnp.dot(latent[:, key_rank:], up[1], preferred_element_type=jnp.float32)
        for g in range(groups):
            values[g] = values_raw[:, g * HEAD : (g + 1) * HEAD].astype(jnp.bfloat16)
        if masked:
            shape = (rows, rows)
            gap = (
                lax.broadcasted_iota(jnp.int32, shape, 0)
                - lax.broadcasted_iota(jnp.int32, shape, 1)
                + distance * rows
            )
            allowed = (gap >= 0) & (gap < WINDOW)
            allowed = jnp.concatenate([allowed.astype(jnp.float32)] * ratio, axis=0)
        for g in range(groups):
            raw = lax.dot_general(
                qs[g], keys[g], (((1,), (1,)), ((), ())), preferred_element_type=jnp.float32
            )
            expo = jnp.exp2(EXP_SCALE * jnp.tanh(raw * (query_scale / soft_cap)))
            if masked:
                expo = expo * allowed
            partial = expo[:, :HEAD]
            for column in range(HEAD, rows, HEAD):
                partial = partial + expo[:, column : column + HEAD]
            denom[g] += partial
            numer[g] += jnp.dot(expo.astype(jnp.bfloat16), values[g], preferred_element_type=jnp.float32)

    attend(seq, 0, True)

    def step(k, carry):
        block = seq - k
        odd = lax.rem(k, 2) == 1

        @pl.when(odd & (k + 1 <= seq))
        def _():
            arrived = block - 1
            chain(arrived).wait_recv()

            @pl.when(has_next)
            def _():
                chain(arrived).start()

            swap(arrived).start()

        @pl.when(odd)
        def _():
            swap(block).wait_recv()

        if total <= WINDOW:
            attend(block, k, False)
        else:
            edge = (k + 1) * rows > WINDOW

            @pl.when(jnp.logical_not(edge))
            def _():
                attend(block, k, False)

            @pl.when(edge & ((k - 1) * rows < WINDOW))
            def _():
                attend(block, k, True)

        return carry

    lax.fori_loop(1, seq + 1, step, 0)

    live_rows = lax.broadcasted_iota(jnp.int32, (rows, HEAD), 0) < live_count
    width = ratio * HEAD
    for g in range(groups):
        result = numer[g] / jnp.sum(denom[g], axis=1, keepdims=True)
        for r in range(ratio):
            column = g * width + r * HEAD
            piece_out = jnp.where(live_rows, result[r * rows : (r + 1) * rows], 0.0)
            out_buf[:, column : column + HEAD] = piece_out.astype(jnp.bfloat16)
        columns = pl.ds(g * width, width)
        local(out_buf.at[:, columns], attended_out.at[0, :, columns], out_sem.at[g]).start()

    def drain(k, carry):
        block = seq - 2 * k

        @pl.when(has_next)
        def _():
            chain(block).wait_send()

        @pl.when((k > 0) | (side == 0))
        def _():
            swap(block).wait_send()

        return carry

    lax.fori_loop(0, seq // 2 + 1, drain, 0)
    for copy in x_copies + y_copies + near_copies + far_copies + [own_copy, up_across, up_mate, up_relay]:
        copy.wait_send()
    latent_copy.wait()
    for g in range(groups):
        columns = pl.ds(g * width, width)
        local(out_buf.at[:, columns], attended_out.at[0, :, columns], out_sem.at[g]).wait()


def body(ring, dp_size, hidden, queries, down_weight, up_weight, lengths):
    _, rows, model_dim = hidden.shape
    shard, rank = down_weight.shape
    kv_width = up_weight.shape[2]
    groups = kv_width // HEAD
    q_width = queries.shape[2]
    ratio = q_width // kv_width
    near, far = angle_tables(rows, ring)
    pieces = piece_count(shard // 2)
    any_spec = pl.BlockSpec(memory_space=pl.ANY)
    vmem_spec = pl.BlockSpec(memory_space=pltpu.VMEM)
    f32, bf16, dma = jnp.float32, jnp.bfloat16, pltpu.SemaphoreType.DMA
    return pl.pallas_call(
        functools.partial(kernel, ring, pieces),
        out_shape=(
            jax.ShapeDtypeStruct((1, rows, rank), bf16),
            jax.ShapeDtypeStruct((1, rows, q_width), bf16),
        ),
        in_specs=[pl.BlockSpec(memory_space=pltpu.SMEM)] + [any_spec] * 4 + [vmem_spec] * 2,
        out_specs=(any_spec, any_spec),
        scratch_shapes=[
            pltpu.VMEM((rows, model_dim), bf16),
            pltpu.VMEM((rows, q_width), bf16),
            pltpu.VMEM((groups, ratio * rows, HEAD), bf16),
            pltpu.VMEM((dp_size, shard, rank), bf16),
            pltpu.VMEM((2, dp_size * up_weight.shape[1], kv_width), bf16),
            pltpu.VMEM((ring, rows, rank), bf16),
            pltpu.VMEM((rows, rank), f32),
            pltpu.VMEM((groups, rows, HEAD), bf16),
            pltpu.VMEM((groups, rows, HEAD), bf16),
            pltpu.VMEM((groups, ratio * rows, HEAD), f32),
            pltpu.VMEM((groups, ratio * rows, HEAD), f32),
            pltpu.VMEM((rows, q_width), bf16),
            dma((4,)),
            dma((pieces,)), dma((pieces,)),
            dma((pieces,)), dma((pieces,)),
            dma((2, pieces)), dma((2, pieces)),
            dma, dma,
            dma((3,)), dma((3,)),
            dma((ring,)), dma((ring,)), dma((ring,)),
            dma((groups + 1,)),
        ],
        compiler_params=pltpu.CompilerParams(
            collective_id=0, has_side_effects=True, vmem_limit_bytes=60 * 1024 * 1024
        ),
    )(lengths, hidden, queries, down_weight, up_weight, jnp.asarray(near), jnp.asarray(far))


def solution(mesh):
    in_specs = (
        P("dp", "seq", None),
        P("dp", "seq", None),
        P("dp", None),
        P(None, "dp", None),
        P("dp"),
    )
    out_specs = (P("dp", "seq", None), P("dp", "seq", None))
    step = functools.partial(body, mesh.shape["seq"], mesh.shape["dp"])
    return jax.shard_map(step, mesh=mesh, in_specs=in_specs, out_specs=out_specs, check_vma=False)
```

```python
import functools
import math

import jax
import jax.numpy as jnp
import numpy as np
from jax import lax
from jax.experimental import pallas as pl
from jax.experimental.pallas import tpu as pltpu
from jax.sharding import PartitionSpec as P

HEAD = 128
WINDOW = 4096
MESH = pl.DeviceIdType.MESH

query_scale = 144.0 ** (-0.5)
soft_cap = 50.0
EXP_SCALE = soft_cap * math.log2(math.e)


def angle_tables(rows, blocks):
    half = HEAD // 2
    freqs = 10000.0 ** (-2.0 * np.arange(half, dtype=np.float64) / HEAD)
    freqs = np.concatenate([freqs, freqs])[None, :]
    sign = np.concatenate([-np.ones(half), np.ones(half)])[None, :]
    near = np.arange(rows, dtype=np.float64)[:, None] * freqs
    far = (rows * np.arange(blocks, dtype=np.float64))[:, None] * freqs
    near = np.stack([np.cos(near), sign * np.sin(near)]).astype(np.float32)
    far = np.stack([np.cos(far), sign * np.sin(far)]).astype(np.float32)
    return near, far


def piece_count(quarter):
    for pieces in (6, 4, 2):
        if quarter % (pieces * 16) == 0:
            return pieces
    return 2


def kernel(
    ring, pieces, lengths_ref, hidden_ref, q_ref, down_ref, up_ref, near_ref, far_ref,
    latent_out, attended_out,
    hid, q_raw, qs, wf, up, lat, acc, keys, values, numer, denom, out_buf,
    local_sem, x_send, x_recv, y_send, y_recv, z_send, z_recv, c_send, c_recv, own_send, own_recv,
    up_send, up_recv, chain_send, pair_send, lat_recv, out_sem,
):
    seq = lax.axis_index("seq")
    dp = lax.axis_index("dp")
    rows = lat.shape[1]
    shard = down_ref.shape[0]
    quarter = shard // 4
    piece = quarter // pieces
    split = pieces // 2
    half_rows = rows // 2
    up_rows = up_ref.shape[1]
    groups = qs.shape[0]
    ratio = qs.shape[1] // rows
    key_rank = lat.shape[2] // 2
    total = ring * rows

    side = lax.rem(seq, 2)
    pair = seq + 1 - 2 * side
    level = lax.rem(seq // 2, 2)
    fellow = seq + 2 - 4 * level
    own_part = 2 * side + level
    pair_part = 2 - 2 * side + level
    fellow_part = 2 * side + 1 - level
    diagonal_part = 3 - own_part
    core = lax.rem(dp, 2)
    mate = dp + 1 - 2 * core
    across = lax.rem(dp + 2, 4)
    diagonal = lax.rem(mate + 2, 4)
    has_next = seq + 2 < ring
    has_prev = seq >= 2

    def local(src, dst, sem):
        return pltpu.make_async_copy(src, dst, sem)

    loads = [
        local(down_ref, wf.at[dp], local_sem.at[0]),
        local(hidden_ref.at[0], hid, local_sem.at[1]),
        local(up_ref, up.at[:, pl.ds(pl.multiple_of(dp * up_rows, up_rows), up_rows), :], local_sem.at[2]),
        local(q_ref.at[0], q_raw, local_sem.at[3]),
    ]
    for load in loads:
        load.start()

    barrier = pltpu.get_barrier_semaphore()

    def greet(device):
        pl.semaphore_signal(barrier, inc=1, device_id=device, device_id_type=MESH)

    greet({"seq": seq, "dp": mate})
    greet({"seq": seq, "dp": across})
    greet({"seq": pair, "dp": dp})

    @pl.when(has_next)
    def _():
        greet({"seq": seq + 2, "dp": dp})

    @pl.when(has_prev)
    def _():
        greet({"seq": seq - 2, "dp": dp})

    pl.semaphore_wait(barrier, 3 + has_next.astype(jnp.int32) + has_prev.astype(jnp.int32))

    def remote(src, dst, send, recv, device):
        return pltpu.make_async_remote_copy(
            src_ref=src, dst_ref=dst, send_sem=send, recv_sem=recv, device_id=device, device_id_type=MESH
        )

    to_mate = {"seq": seq, "dp": mate}
    to_across = {"seq": seq, "dp": across}
    to_pair = {"seq": pair, "dp": dp}
    to_fellow = {"seq": fellow, "dp": dp}
    to_next = {"seq": lax.rem(seq + 2, ring), "dp": dp}

    def part(which, index):
        return pl.ds(pl.multiple_of(which * quarter + index * piece, 16), piece)

    def x_copy(index):
        return remote(
            down_ref.at[part(own_part, index)], wf.at[dp, part(own_part, index)],
            x_send.at[index], x_recv.at[index], to_across,
        )

    def y_copy(which, slot):
        view = wf.at[across, part(which, slot % pieces)]
        return remote(view, view, y_send.at[slot], y_recv.at[slot], to_pair)

    def z_copy(which, slot):
        view = wf.at[across, part(which, slot % pieces)]
        return remote(view, view, z_send.at[slot], z_recv.at[slot], to_fellow)

    def c_copy(slot, which, index):
        view = wf.at[across, part(which, index)]
        return remote(view, view, c_send.at[slot, index], c_recv.at[slot, index], to_mate)

    x_copies = [x_copy(i) for i in range(pieces)]
    for copy in x_copies:
        copy.start()
    own_copy = remote(down_ref, wf.at[dp], own_send, own_recv, to_mate)
    own_copy.start()

    def up_view(owner):
        return up.at[:, pl.ds(pl.multiple_of(owner * up_rows, up_rows), up_rows), :]

    up_across = remote(up_ref, up_view(dp), up_send.at[0], up_recv.at[0], to_across)
    up_across.start()
    up_mate = remote(up_ref, up_view(dp), up_send.at[1], up_recv.at[1], to_mate)
    up_mate.start()

    loads[3].wait()
    for g in range(groups):
        for r in range(ratio):
            column = (g * ratio + r) * HEAD
            qs[g, r * rows : (r + 1) * rows, :] = q_raw[:, column : column + HEAD]
    numer[...] = jnp.zeros_like(numer)
    denom[...] = jnp.zeros_like(denom)

    def project(owner):
        columns = pl.ds(pl.multiple_of(owner * shard, 128), shard)
        return jnp.dot(hid[:, columns], wf[owner], preferred_element_type=jnp.float32)

    loads[1].wait()
    loads[0].wait()
    acc[...] = project(dp)

    y_copies = [y_copy(own_part, i) for i in range(pieces)]
    z_copies = [z_copy(own_part, i) for i in range(pieces)]
    relays = [
        y_copy(fellow_part, pieces + i) if i < split else z_copy(pair_part, pieces + i)
        for i in range(pieces)
    ]
    mate_copies = [
        [c_copy(slot, which, i) for i in range(pieces)]
        for slot, which in enumerate((own_part, pair_part, fellow_part, diagonal_part))
    ]

    def pass_on(i):
        y_copies[i].wait_recv()
        if i >= split:
            relays[i].start()
        mate_copies[1][i].start()
        z_copies[i].wait_recv()
        if i < split:
            relays[i].start()
        mate_copies[2][i].start()

    for i in range(pieces):
        x_copies[i].wait_recv()
        y_copies[i].start()
        z_copies[i].start()
        mate_copies[0][i].start()
        if i >= 1:
            pass_on(i - 1)
    pass_on(pieces - 1)
    own_copy.wait_recv()
    acc[...] += project(mate)
    for i in range(pieces):
        relays[i].wait_recv()
        mate_copies[3][i].start()
    acc[...] += project(across)
    for copies in mate_copies:
        for copy in copies:
            copy.wait_recv()
    live_count = lengths_ref[0] - seq * rows
    total_rows = acc[...] + project(diagonal)
    live = lax.broadcasted_iota(jnp.int32, total_rows.shape, 0) < live_count
    lat[seq] = jnp.where(live, total_rows, 0.0).astype(jnp.bfloat16)

    def chain(block, part_index):
        view = lat.at[block, pl.ds(part_index * half_rows, half_rows)]
        return remote(
            view, view, chain_send.at[block, part_index], lat_recv.at[block, part_index], to_next
        )

    def swap(block, part_index):
        view = lat.at[block, pl.ds(part_index * half_rows, half_rows)]
        return remote(
            view, view, pair_send.at[block, part_index], lat_recv.at[block, part_index], to_pair
        )

    @pl.when(has_next)
    def _():
        chain(seq, 0).start()
        chain(seq, 1).start()

    @pl.when(side == 0)
    def _():
        swap(seq, 0).start()
        swap(seq, 1).start()

    latent_copy = local(lat.at[seq], latent_out.at[0], out_sem.at[groups])
    latent_copy.start()

    up_mate.wait_recv()
    up_across.wait_recv()
    up_relay = remote(up_view(across), up_view(across), up_send.at[2], up_recv.at[2], to_mate)
    up_relay.start()
    loads[2].wait()
    up_relay.wait_recv()

    def attend(block, distance, masked):
        latent = lat[block]
        near_cos, near_sin = near_ref[0], near_ref[1]
        far_cos = far_ref[0, pl.ds(block, 1), :]
        far_sin = far_ref[1, pl.ds(block, 1), :]
        cosine = near_cos * far_cos - near_sin * far_sin
        sine = near_sin * far_cos + near_cos * far_sin
        keys_raw = jnp.dot(latent[:, :key_rank], up[0], preferred_element_type=jnp.float32)
        for g in range(groups):
            head = keys_raw[:, g * HEAD : (g + 1) * HEAD]
            turned = head * cosine + pltpu.roll(head, HEAD // 2, 1) * sine
            keys[g] = turned.astype(jnp.bfloat16)
        values_raw = jnp.dot(latent[:, key_rank:], up[1], preferred_element_type=jnp.float32)
        for g in range(groups):
            values[g] = values_raw[:, g * HEAD : (g + 1) * HEAD].astype(jnp.bfloat16)
        if masked:
            shape = (rows, rows)
            gap = (
                lax.broadcasted_iota(jnp.int32, shape, 0)
                - lax.broadcasted_iota(jnp.int32, shape, 1)
                + distance * rows
            )
            allowed = (gap >= 0) & (gap < WINDOW)
            allowed = jnp.concatenate([allowed.astype(jnp.float32)] * ratio, axis=0)
        for g in range(groups):
            raw = lax.dot_general(
                qs[g], keys[g], (((1,), (1,)), ((), ())), preferred_element_type=jnp.float32
            )
            expo = jnp.exp2(EXP_SCALE * jnp.tanh(raw * (query_scale / soft_cap)))
            if masked:
                expo = expo * allowed
            partial = expo[:, :HEAD]
            for column in range(HEAD, rows, HEAD):
                partial = partial + expo[:, column : column + HEAD]
            denom[g] += partial
            numer[g] += jnp.dot(expo.astype(jnp.bfloat16), values[g], preferred_element_type=jnp.float32)

    attend(seq, 0, True)

    def step(k, carry):
        block = seq - k
        odd = lax.rem(k, 2) == 1

        @pl.when(odd & (k + 1 <= seq))
        def _():
            arrived = block - 1
            for h in range(2):
                chain(arrived, h).wait_recv()

                @pl.when(has_next)
                def _():
                    chain(arrived, h).start()

                if h == 0:
                    swap(arrived, h).start()
                else:

                    @pl.when(arrived > 0)
                    def _():
                        swap(arrived, h).start()

        @pl.when(odd)
        def _():
            swap(block, 0).wait_recv()
            swap(block, 1).wait_recv()

            @pl.when((block == 0) & has_next & (side == 1))
            def _():
                chain(block, 1).start()

        if total <= WINDOW:
            attend(block, k, False)
        else:
            edge = (k + 1) * rows > WINDOW

            @pl.when(jnp.logical_not(edge))
            def _():
                attend(block, k, False)

            @pl.when(edge & ((k - 1) * rows < WINDOW))
            def _():
                attend(block, k, True)

        return carry

    lax.fori_loop(1, seq + 1, step, 0)

    live_rows = lax.broadcasted_iota(jnp.int32, (rows, HEAD), 0) < live_count
    width = ratio * HEAD
    for g in range(groups):
        result = numer[g] / jnp.sum(denom[g], axis=1, keepdims=True)
        for r in range(ratio):
            column = g * width + r * HEAD
            piece_out = jnp.where(live_rows, result[r * rows : (r + 1) * rows], 0.0)
            out_buf[:, column : column + HEAD] = piece_out.astype(jnp.bfloat16)
        columns = pl.ds(g * width, width)
        local(out_buf.at[:, columns], attended_out.at[0, :, columns], out_sem.at[g]).start()

    def drain(k, carry):
        block = seq - 2 * k

        @pl.when(has_next)
        def _():
            chain(block, 0).wait_send()
            chain(block, 1).wait_send()

        @pl.when((k > 0) | (side == 0))
        def _():
            swap(block, 0).wait_send()

        @pl.when((side == 1) & (k > 0) | (side == 0) & ((block > 0) | (seq == 0)))
        def _():
            swap(block, 1).wait_send()

        return carry

    lax.fori_loop(0, seq // 2 + 1, drain, 0)

    @pl.when(has_next & (side == 1))
    def _():
        chain(0, 1).wait_send()

    for copy in x_copies + y_copies + z_copies + relays + sum(mate_copies, []) + [own_copy, up_across, up_mate, up_relay]:
        copy.wait_send()
    latent_copy.wait()
    for g in range(groups):
        columns = pl.ds(g * width, width)
        local(out_buf.at[:, columns], attended_out.at[0, :, columns], out_sem.at[g]).wait()


def body(ring, dp_size, hidden, queries, down_weight, up_weight, lengths):
    _, rows, model_dim = hidden.shape
    shard, rank = down_weight.shape
    kv_width = up_weight.shape[2]
    groups = kv_width // HEAD
    q_width = queries.shape[2]
    ratio = q_width // kv_width
    near, far = angle_tables(rows, ring)
    pieces = piece_count(shard // 4)
    any_spec = pl.BlockSpec(memory_space=pl.ANY)
    vmem_spec = pl.BlockSpec(memory_space=pltpu.VMEM)
    f32, bf16, dma = jnp.float32, jnp.bfloat16, pltpu.SemaphoreType.DMA
    return pl.pallas_call(
        functools.partial(kernel, ring, pieces),
        out_shape=(
            jax.ShapeDtypeStruct((1, rows, rank), bf16),
            jax.ShapeDtypeStruct((1, rows, q_width), bf16),
        ),
        in_specs=[pl.BlockSpec(memory_space=pltpu.SMEM)] + [any_spec] * 4 + [vmem_spec] * 2,
        out_specs=(any_spec, any_spec),
        scratch_shapes=[
            pltpu.VMEM((rows, model_dim), bf16),
            pltpu.VMEM((rows, q_width), bf16),
            pltpu.VMEM((groups, ratio * rows, HEAD), bf16),
            pltpu.VMEM((dp_size, shard, rank), bf16),
            pltpu.VMEM((2, dp_size * up_weight.shape[1], kv_width), bf16),
            pltpu.VMEM((ring, rows, rank), bf16),
            pltpu.VMEM((rows, rank), f32),
            pltpu.VMEM((groups, rows, HEAD), bf16),
            pltpu.VMEM((groups, rows, HEAD), bf16),
            pltpu.VMEM((groups, ratio * rows, HEAD), f32),
            pltpu.VMEM((groups, ratio * rows, HEAD), f32),
            pltpu.VMEM((rows, q_width), bf16),
            dma((4,)),
            dma((pieces,)), dma((pieces,)),
            dma((2 * pieces,)), dma((2 * pieces,)),
            dma((2 * pieces,)), dma((2 * pieces,)),
            dma((4, pieces)), dma((4, pieces)),
            dma, dma,
            dma((3,)), dma((3,)),
            dma((ring, 2)), dma((ring, 2)), dma((ring, 2)),
            dma((groups + 1,)),
        ],
        compiler_params=pltpu.CompilerParams(
            collective_id=0, has_side_effects=True, vmem_limit_bytes=60 * 1024 * 1024
        ),
    )(lengths, hidden, queries, down_weight, up_weight, jnp.asarray(near), jnp.asarray(far))


def solution(mesh):
    in_specs = (
        P("dp", "seq", None),
        P("dp", "seq", None),
        P("dp", None),
        P(None, "dp", None),
        P("dp"),
    )
    out_specs = (P("dp", "seq", None), P("dp", "seq", None))
    step = functools.partial(body, mesh.shape["seq"], mesh.shape["dp"])
    return jax.shard_map(step, mesh=mesh, in_specs=in_specs, out_specs=out_specs, check_vma=False)
```
